32 devices in a mesh: comp: 2 (over core), tgt: 4 (over y, x), src: 4 (over z).
Axes of the slice: x: 2, y: 2, z: 4, core: 2. Of those that a mesh axis runs over, the one named last changes fastest.
Arguments:
- field: bfloat16 [3, 32, 8192], P(None, None, ('tgt', 'src')), may hold values from -6 to 6
- dest_group: int32 [4096, 1], P(('comp', 'tgt', 'src')), may hold values from 0 to 3; in each aligned block of 128 rows (0 to 127, 128 to 255, ...) at most 64 rows name the same one
- src_local: int32 [4096], P(('comp', 'tgt', 'src')), may hold values from 0 to 1
- ranks: int32 [4096], P(('comp', 'tgt', 'src')), may hold values from 8 to 64
- mixing: float32 [4096, 3, 3], P(('comp', 'tgt', 'src')), may hold values from -5 to 5
- v_factor: bfloat16 [4096, 64, 256], P(('comp', 'tgt', 'src')), may hold values from -0.375 to 0.375
- u_factor: bfloat16 [8192, 64, 256], P(('comp', 'tgt', 'src')), may hold values from -0.0625 to 0.0625
- slot_cluster: int32 [8192], P(('comp', 'tgt', 'src')), may hold values from 0 to 7
- near_src: int32 [128], P(('comp', 'tgt', 'src')), may hold values from 0 to 1
- near_tgt: int32 [128], P(('comp', 'tgt', 'src')), may hold values from 0 to 7
- near_mixing: float32 [128, 3, 3], P(('comp', 'tgt', 'src')), may hold values from -5 to 5
- near_matrix: bfloat16 [128, 256, 256], P(('comp', 'tgt', 'src')), may hold values from -0.1875 to 0.1875
Outputs:
- result: float32 [3, 32, 8192], P(None, None, ('comp', 'tgt', 'src'))
The draws below stay inside these ranges and needn't reach their ends.
Inputs may be any that keep to these rules, and one draw needn't show every extreme that they name: `dest_group`: among the 128 blocks of one device at most 64 name the same target group, and in every draw some device has exactly 64 blocks to one group.
All inputs are finite; a program needn't handle non-finite values.
Results may differ from the reference program's by a relative error of at most 0.0018.
Values may be sent and summed in bfloat16 or wider, within the bound.
A program may use at most 128 MiB of HBM per device.

```python
import math
import jax
import jax.numpy as jnp
import numpy as np
from jax import lax

CL = 256
R = 64
RHS = 32
CLU_DEV = 2
BLK_DEV = 128
NEAR_DEV = 4
CAP = 64
NPTS = 8192
NBLK = 4096
USLOTS = 8192
NNEAR = 128
N_COMP = 2
N_TGT = 4
N_SRC = 4


def touch_ends(drawn, key, least, largest):
    longest = drawn.shape.index(max(drawn.shape))
    spots = []
    for shift in (0, 1):
        where = [jax.random.randint(jax.random.fold_in(key, axis), (), 0, length) for axis, length in enumerate(drawn.shape)]
        where[longest] = (where[longest] + shift) % drawn.shape[longest]
        spots.append(tuple(where))
    return drawn.at[spots[0]].set(least).at[spots[1]].set(largest)


def steps_of(own_key, dims, shards, smallest, largest):
    level = 1.0
    for axis_at, shards_of in shards:
        steps = jax.random.uniform(jax.random.fold_in(jax.random.fold_in(own_key, 6), axis_at), (shards_of,), jnp.float32, smallest / len(shards), largest / len(shards))
        level = level * jnp.repeat(jnp.exp(steps), dims[axis_at] // shards_of).reshape((-1,) + (1,) * (len(dims) - 1 - axis_at))
    return level


def assign_block(own_key, own, number, rows, count, top, reach, skew):
    order = jax.random.permutation(own_key, count)
    crowded, usual = load_shares(count, rows * top, reach, skew, True), load_shares(count, rows * top, reach, skew, False)
    places = jnp.arange(count)

    def named(sizes, offset_by):
        used = int((sizes > 0).sum())
        fixed = max(1, used // 4)
        shifted = fixed + (places - fixed + offset_by * (used - fixed)) % max(1, count - fixed)
        return jnp.zeros((count,), jnp.int32).at[order[jnp.where(places < fixed, places, shifted)]].set(jnp.asarray(sizes, jnp.int32))

    sizes = jnp.where(number % 4 == 0, named(crowded, number // 4), named(usual, number - number // 4 - 1))
    mixed = jax.random.permutation(jax.random.fold_in(own, 3), count)
    donor, taker = mixed[0:count // 2 * 2:2], mixed[1:count // 2 * 2:2]
    room = jnp.minimum(sizes[donor] - 1, reach - sizes[taker]) // 2
    room = jnp.where((donor == order[0]) | (taker == order[0]) | (sizes[taker] == 0), 0, jnp.maximum(room, 0))
    shifted = jax.random.randint(jax.random.fold_in(own, 4), (count // 2,), 0, 1 << 20) % (room + 1)
    sizes = sizes.at[donor].add(-shifted).at[taker].add(shifted)
    members = jnp.searchsorted(jnp.cumsum(sizes), jnp.arange(rows * top), side="right").astype(jnp.int32)
    grid = members.reshape(top, rows).T
    grid = grid[jax.random.permutation(jax.random.fold_in(own, 1), rows)]
    offset_by = jax.random.randint(jax.random.fold_in(own, 2), (rows, 1), 0, top)
    return jnp.take_along_axis(grid, (jnp.arange(top)[None, :] + offset_by) % top, axis=1)


def load_shares(count, total, most, lean, full):
    portions = [(1 << 20) // math.isqrt(standing ** lean) + 1 for standing in range(1, count + 1)]
    largest = most if full else min(most, max(-(-total // count), total * portions[0] // sum(portions)))
    least = 1 if total - largest >= count - 1 else 0
    counts, surplus = [largest] + [least] * (count - 1), total - largest - least * (count - 1)
    while surplus > 0:
        candidates = [i for i in range(1, count) if counts[i] < largest] or [i for i in range(1, count) if counts[i] < most]
        whole, left = sum([portions[i] for i in candidates]), surplus
        for i in candidates:
            addition = min(most - counts[i], max(1, left * portions[i] // whole), surplus)
            counts[i] = counts[i] + addition
            surplus = surplus - addition
    return np.array(counts)


def noise(own_key, extent, scale, reach, shards=(), kind=jnp.bfloat16):
    loudness = steps_of(own_key, extent, shards, -0.22, 0.18) if shards else 1.0
    values = jax.random.normal(own_key, extent, jnp.float32) * scale * loudness
    return jnp.minimum(jnp.maximum(values, -reach), reach).astype(kind)


def setup_inputs(seed: int = 0) -> dict:
    streams_of = jax.random.split(jax.random.key(seed), 13)
    field = noise(streams_of[0], (3, RHS, NPTS), 1.0, 6.0, ((2, 16),))
    dest_group_keys = jax.random.split(jax.random.fold_in(streams_of[1], 1), NBLK // BLK_DEV)
    dest_group_turns = jax.random.permutation(jax.random.fold_in(streams_of[1], 3), NBLK // BLK_DEV)
    dest_group = jax.vmap(lambda own, number: assign_block(jax.random.fold_in(streams_of[1], 2), own, number, BLK_DEV, N_TGT, 1, CAP, 2))(dest_group_keys, dest_group_turns).reshape((NBLK, 1))
    src_local = touch_ends(jax.random.randint(streams_of[2], (NBLK,), 0, CLU_DEV), jax.random.fold_in(streams_of[2], 1), 0, CLU_DEV - 1).astype(jnp.int32)
    ranks = touch_ends(jax.random.randint(streams_of[3], (NBLK,), max(1, R // 8), R + 1), jax.random.fold_in(streams_of[3], 1), max(1, R // 8), R).astype(jnp.int32)
    mixing = noise(streams_of[4], (NBLK, 3, 3), 1.0, 5.0, ((0, 32),), jnp.float32)
    v_factor = noise(streams_of[5], (NBLK, R, CL), CL ** -0.5, 0.375, ((0, 32),))
    u_factor = noise(streams_of[6], (USLOTS, R, CL), (R * BLK_DEV) ** -0.5, 0.0625, ((0, 32),))
    slot_cluster = touch_ends(jax.random.randint(streams_of[7], (USLOTS,), 0, CLU_DEV * N_SRC), jax.random.fold_in(streams_of[7], 1), 0, (CLU_DEV * N_SRC) - 1).astype(jnp.int32)
    near_src = touch_ends(jax.random.randint(streams_of[8], (NNEAR,), 0, CLU_DEV), jax.random.fold_in(streams_of[8], 1), 0, CLU_DEV - 1).astype(jnp.int32)
    near_tgt = touch_ends(jax.random.randint(streams_of[9], (NNEAR,), 0, CLU_DEV * N_SRC), jax.random.fold_in(streams_of[9], 1), 0, (CLU_DEV * N_SRC) - 1).astype(jnp.int32)
    near_mixing = noise(streams_of[10], (NNEAR, 3, 3), 1.0, 5.0, ((0, 32),), jnp.float32)
    near_matrix = noise(streams_of[11], (NNEAR, CL, CL), (CL * NEAR_DEV) ** -0.5, 0.1875, ((0, 32),))
    return dict(field=field, dest_group=dest_group, src_local=src_local, ranks=ranks, mixing=mixing, v_factor=v_factor, u_factor=u_factor, slot_cluster=slot_cluster, near_src=near_src, near_tgt=near_tgt, near_mixing=near_mixing, near_matrix=near_matrix)


def reference(field, dest_group, src_local, ranks, mixing, v_factor, u_factor, slot_cluster, near_src, near_tgt, near_mixing, near_matrix):
    devices = N_COMP * N_TGT * N_SRC
    channels = 3 * RHS
    half_owned = CLU_DEV // 2
    source_count = N_TGT * N_SRC * CLU_DEV
    sources = jnp.transpose(field.reshape(channels, source_count, CL), (1, 0, 2))
    device_ids = jnp.arange(devices, dtype=jnp.int32)
    comp_of = device_ids // (N_TGT * N_SRC)
    tgt_of = (device_ids // N_SRC) % N_TGT
    src_of = device_ids % N_SRC
    destination = dest_group.reshape(devices, BLK_DEV).astype(jnp.int32)
    member = (destination[:, :, None] == jnp.arange(N_TGT, dtype=jnp.int32)[None, None, :]).astype(jnp.int32)
    position = jnp.sum(jnp.cumsum(member, axis=1) * member, axis=2) - 1
    sender_row = tgt_of * N_SRC + src_of
    source_ids = sender_row[:, None] * CLU_DEV + src_local.reshape(devices, BLK_DEV)
    receiver = (comp_of[:, None] * N_TGT + destination) * N_SRC + src_of[:, None]
    u_rows = (receiver * (N_TGT * CAP) + tgt_of[:, None] * CAP + position).astype(jnp.int32)
    within = slot_cluster[u_rows.reshape(-1)].reshape(devices, BLK_DEV)

    def global_target(group, inner):
        comp_part = inner // (N_SRC * half_owned)
        src_part = (inner // half_owned) % N_SRC
        local_part = inner % half_owned
        return (((comp_part * N_TGT + group) * N_SRC + src_part) * half_owned + local_part).astype(jnp.int32)

    far_targets = global_target(destination, within)
    near_targets = global_target(jnp.broadcast_to(tgt_of[:, None], (devices, NEAR_DEV)), near_tgt.reshape(devices, NEAR_DEV))
    near_sources = sender_row[:, None] * CLU_DEV + near_src.reshape(devices, NEAR_DEV)
    total = jnp.zeros((N_COMP * N_TGT * N_SRC * half_owned, channels, CL), jnp.float32)

    def far_step(carry, items):
        source_rows, rank_row, mix_row, v_rows, u_index, target_rows = items
        inputs = sources[source_rows].astype(jnp.float32)
        coefficients = jnp.einsum("bfp,brp->bfr", inputs, v_rows.astype(jnp.float32))
        rank_mask = (jnp.arange(R, dtype=jnp.int32)[None, :] < rank_row[:, None]).astype(jnp.float32)
        coefficients = (coefficients * rank_mask[:, None, :]).reshape(BLK_DEV, 3, RHS, R)
        mixed_coef = jnp.einsum("bcd,bdsr->bcsr", mix_row.astype(jnp.float32), coefficients)
        sent = lax.optimization_barrier(mixed_coef.reshape(BLK_DEV, channels, R).astype(jnp.bfloat16))
        basis = u_factor[u_index].astype(jnp.float32)
        contrib = jnp.einsum("bfr,brq->bfq", sent.astype(jnp.float32), basis)
        return carry.at[target_rows].add(contrib), None

    total, unused = lax.scan(far_step, total, (source_ids, ranks.reshape(devices, BLK_DEV), mixing.reshape(devices, BLK_DEV, 3, 3), v_factor.reshape(devices, BLK_DEV, R, CL), u_rows, far_targets))

    def near_step(carry, items):
        source_rows, mix_row, dense_rows, target_rows = items
        inputs = sources[source_rows].astype(jnp.float32)
        dense_out = jnp.einsum("nfp,nqp->nfq", inputs, dense_rows.astype(jnp.float32)).reshape(NEAR_DEV, 3, RHS, CL)
        mixed_near = jnp.einsum("ncd,ndsq->ncsq", mix_row.astype(jnp.float32), dense_out).reshape(NEAR_DEV, channels, CL)
        return carry.at[target_rows].add(mixed_near), None

    total, unused = lax.scan(near_step, total, (near_sources, near_mixing.reshape(devices, NEAR_DEV, 3, 3), near_matrix.reshape(devices, NEAR_DEV, CL, CL), near_targets))
    return jnp.transpose(total, (1, 0, 2)).reshape(3, RHS, NPTS)
```

```python
import functools

import jax
import jax.numpy as jnp
from jax import lax
from jax.experimental import pallas as pl
from jax.experimental.pallas import tpu as pltpu
from jax.sharding import PartitionSpec as P

NT = (((1,), (1,)), ((), ()))


def mix_rows(weights, value, components):
    rows = value.shape[0] // components
    parts = [value[d * rows : (d + 1) * rows] for d in range(components)]
    mixed = []
    for c in range(components):
        total = weights[c][0] * parts[0]
        for d in range(1, components):
            total = total + weights[c][d] * parts[d]
        mixed.append(total)
    return jnp.concatenate(mixed, axis=0)


def coef_kernel(components, dest, src, ranks, mix, x_ref, v_ref, out_ref, order, count):
    groups, pairs, channels, lanes = out_ref.shape
    width = lanes // 2
    blocks = v_ref.shape[0]
    clusters = x_ref.shape[0] // channels
    capacity = 2 * pairs
    unroll = 4 if pairs % 4 == 0 else 1

    def clear(g, carry):
        count[g] = 0
        return carry

    lax.fori_loop(0, groups, clear, 0)

    def place(b, carry):
        g = dest[b]
        k = count[g]
        order[g * capacity + k] = b
        count[g] = k + 1
        return carry

    lax.fori_loop(0, blocks, place, 0)
    lane = lax.broadcasted_iota(jnp.int32, (1, lanes), 1)
    first = lane < width
    rank_at = lane % width

    def group(g, carry):
        used = count[g]

        def one(m):
            k = 2 * m
            b0 = jnp.where(k < used, order[g * capacity + k], 0)
            b1 = jnp.where(k + 1 < used, order[g * capacity + k + 1], 0)
            r0 = jnp.where(k < used, ranks[b0], 0)
            r1 = jnp.where(k + 1 < used, ranks[b1], 0)
            v = jnp.concatenate([v_ref[b0], v_ref[b1]], axis=0)
            y = lax.dot_general(x_ref[...], v, NT, preferred_element_type=jnp.float32)
            chosen = jnp.where(first, src[b0], src[b1])
            coef = y[:channels]
            for s in range(1, clusters):
                coef = jnp.where(chosen == s, y[s * channels : (s + 1) * channels], coef)
            coef = jnp.where(rank_at < jnp.where(first, r0, r1), coef, 0.0)
            square = components * components
            weights = [
                [
                    jnp.where(
                        first,
                        mix[b0 * square + c * components + d],
                        mix[b1 * square + c * components + d],
                    )
                    for d in range(components)
                ]
                for c in range(components)
            ]
            out_ref[g, m] = mix_rows(weights, coef, components).astype(jnp.bfloat16)

        def several(step, carry):
            for u in range(unroll):
                one(step * unroll + u)
            return carry

        steps = (used + 2 * unroll - 1) // (2 * unroll)
        lax.fori_loop(0, steps, several, 0)

        def blank(m, carry):
            out_ref[g, m] = jnp.zeros((channels, lanes), jnp.bfloat16)
            return carry

        lax.fori_loop(steps * unroll, pairs, blank, 0)
        return carry

    lax.fori_loop(0, groups, group, 0)


def near_kernel(components, near_src, near_tgt, near_mix, x_ref, matrix_ref, out_ref):
    channels = out_ref.shape[1]
    square = components * components
    out_ref[...] = jnp.zeros_like(out_ref)
    for n in range(matrix_ref.shape[0]):
        x = x_ref[pl.ds(pl.multiple_of(near_src[n] * channels, 32), channels), :]
        y = lax.dot_general(x, matrix_ref[n], NT, preferred_element_type=jnp.float32)
        weights = [
            [near_mix[n * square + c * components + d] for d in range(components)]
            for c in range(components)
        ]
        out_ref[near_tgt[n]] += mix_rows(weights, y, components)


def far_kernel(cluster, near_ref, got_ref, u_ref, out_ref):
    step = pl.program_id(0)
    pairs, channels, lanes = got_ref.shape
    first = lax.broadcasted_iota(jnp.int32, (channels, lanes), 1) < lanes // 2
    unroll = 4 if pairs % 4 == 0 else 1

    @pl.when(step == 0)
    def _():
        out_ref[...] = near_ref[...]

    def several(at, carry):
        done = []
        for u in range(unroll):
            m = at * unroll + u
            a = got_ref[m]
            zero = jnp.zeros_like(a)
            both = jnp.concatenate(
                [jnp.where(first, a, zero), jnp.where(first, zero, a)], axis=0
            )
            done.append(
                jnp.dot(both, u_ref[m], preferred_element_type=jnp.float32)
            )
        for u in range(unroll):
            k = 2 * (step * pairs + at * unroll + u)
            out_ref[cluster[k]] += done[u][:channels]
            out_ref[cluster[k + 1]] += done[u][channels:]
        return carry

    lax.fori_loop(0, pairs // unroll, several, 0)


def body(
    field,
    dest_group,
    src_local,
    ranks,
    mixing,
    v_factor,
    u_factor,
    slot_cluster,
    near_src,
    near_tgt,
    near_mixing,
    near_matrix,
):
    groups = lax.axis_size("tgt")
    shards = lax.axis_size("src")
    pairing = lax.axis_size("comp")
    blocks, rank_width, cluster_size = v_factor.shape
    components, vectors, points = field.shape
    channels = components * vectors
    owned = points // cluster_size
    slot_count = u_factor.shape[0]
    capacity = slot_count // groups
    targets = owned * shards
    sources = field.reshape(channels, owned, cluster_size).transpose(1, 0, 2)
    sources = sources.reshape(owned * channels, cluster_size)
    smem = pl.BlockSpec(memory_space=pltpu.SMEM)
    vmem = pl.BlockSpec(memory_space=pltpu.VMEM)
    lanes = 2 * rank_width

    outgoing = pl.pallas_call(
        functools.partial(coef_kernel, components),
        out_shape=jax.ShapeDtypeStruct((groups, capacity // 2, channels, lanes), jnp.bfloat16),
        in_specs=[smem] * 4 + [vmem] * 2,
        out_specs=vmem,
        scratch_shapes=[
            pltpu.SMEM((slot_count,), jnp.int32),
            pltpu.SMEM((groups,), jnp.int32),
        ],
        name="coef",
    )(dest_group.reshape(-1), src_local, ranks, mixing.reshape(-1), sources, v_factor)

    incoming = lax.all_to_all(outgoing, "tgt", split_axis=0, concat_axis=0, tiled=True)

    near_part = pl.pallas_call(
        functools.partial(near_kernel, components),
        out_shape=jax.ShapeDtypeStruct((targets, channels, cluster_size), jnp.float32),
        in_specs=[smem] * 3 + [vmem] * 2,
        out_specs=vmem,
        cost_estimate=pl.CostEstimate(
            flops=2 * near_matrix.size * channels, bytes_accessed=3000000, transcendentals=0
        ),
        name="near",
    )(near_src, near_tgt, near_mixing.reshape(-1), sources, near_matrix)

    pair_count = slot_count // 2
    chunk = 16 if pair_count % 16 == 0 else capacity // 2
    total = pl.pallas_call(
        far_kernel,
        grid=(pair_count // chunk,),
        out_shape=jax.ShapeDtypeStruct((targets, channels, cluster_size), jnp.float32),
        in_specs=[
            smem,
            vmem,
            pl.BlockSpec((chunk, channels, lanes), lambda i: (i, 0, 0)),
            pl.BlockSpec((chunk, lanes, cluster_size), lambda i: (i, 0, 0)),
        ],
        out_specs=vmem,
        compiler_params=pltpu.CompilerParams(dimension_semantics=("arbitrary",)),
        name="far",
    )(
        slot_cluster,
        near_part,
        incoming.reshape(pair_count, channels, lanes),
        u_factor.reshape(pair_count, lanes, cluster_size),
    )

    members = pairing * shards
    kept = targets // members
    pieces = total.reshape(members, kept, channels, cluster_size)
    passed = lax.all_to_all(
        pieces.astype(jnp.bfloat16), ("comp", "src"), split_axis=0, concat_axis=0, tiled=True
    )
    me = lax.axis_index("comp") * shards + lax.axis_index("src")
    own = lax.dynamic_index_in_dim(pieces, me, 0, keepdims=False)
    other = (jnp.arange(members) != me)[:, None, None, None]
    summed = own + jnp.sum(jnp.where(other, passed.astype(jnp.float32), 0.0), axis=0)
    return summed.transpose(1, 0, 2).reshape(components, vectors, kept * cluster_size)


def solution(mesh):
    placed = (
        P(None, None, ("tgt", "src")),
        P(("comp", "tgt", "src"), None),
        P(("comp", "tgt", "src")),
        P(("comp", "tgt", "src")),
        P(("comp", "tgt", "src"), None, None),
        P(("comp", "tgt", "src"), None, None),
        P(("comp", "tgt", "src"), None, None),
        P(("comp", "tgt", "src")),
        P(("comp", "tgt", "src")),
        P(("comp", "tgt", "src")),
        P(("comp", "tgt", "src"), None, None),
        P(("comp", "tgt", "src"), None, None),
    )
    return jax.shard_map(
        body,
        mesh=mesh,
        in_specs=placed,
        out_specs=P(None, None, ("comp", "tgt", "src")),
        check_vma=False,
    )
```

```python
import functools

import jax
import jax.numpy as jnp
from jax import lax
from jax.experimental import pallas as pl
from jax.experimental.pallas import tpu as pltpu
from jax.sharding import PartitionSpec as P


NT = (((1,), (1,)), ((), ()))


def mix_rows(weights, value, components):
    rows = value.shape[0] // components
    parts = [value[d * rows : (d + 1) * rows] for d in range(components)]
    mixed = []
    for c in range(components):
        total = weights[c][0] * parts[0]
        for d in range(1, components):
            total = total + weights[c][d] * parts[d]
        mixed.append(total)
    return jnp.concatenate(mixed, axis=0)


def split_clusters(field_ref, x_ref):
    channels = field_ref.shape[0]
    clusters = x_ref.shape[0] // channels
    size = x_ref.shape[1]
    for s in range(clusters):
        x_ref[pl.ds(s * channels, channels), :] = field_ref[:, s * size : (s + 1) * size]


def coef_kernel(components, groups, offsets, me, dest, src, ranks, mix, field_ref, v_ref, *rest):
    outs = rest[: len(offsets)]
    x_ref, order, count = rest[len(offsets) :]
    pairs, channels, lanes = outs[0].shape
    width = lanes // 2
    blocks = v_ref.shape[0]
    clusters = x_ref.shape[0] // channels
    capacity = 2 * pairs
    unroll = 4 if pairs % 4 == 0 else 1
    split_clusters(field_ref, x_ref)

    def clear(g, carry):
        count[g] = 0
        return carry

    lax.fori_loop(0, groups, clear, 0)

    def place(b, carry):
        g = dest[b]
        k = count[g]
        order[g * capacity + k] = b
        count[g] = k + 1
        return carry

    lax.fori_loop(0, blocks, place, 0)
    lane = lax.broadcasted_iota(jnp.int32, (1, lanes), 1)
    first = lane < width
    rank_at = lane % width
    square = components * components

    def one(out_ref, g, used, m):
        k = 2 * m
        b0 = jnp.where(k < used, order[g * capacity + k], 0)
        b1 = jnp.where(k + 1 < used, order[g * capacity + k + 1], 0)
        r0 = jnp.where(k < used, ranks[b0], 0)
        r1 = jnp.where(k + 1 < used, ranks[b1], 0)
        v = jnp.concatenate([v_ref[b0], v_ref[b1]], axis=0)
        y = lax.dot_general(x_ref[...], v, NT, preferred_element_type=jnp.float32)
        chosen = jnp.where(first, src[b0], src[b1])
        coef = y[:channels]
        for s in range(1, clusters):
            coef = jnp.where(chosen == s, y[s * channels : (s + 1) * channels], coef)
        coef = jnp.where(rank_at < jnp.where(first, r0, r1), coef, 0.0)
        weights = [
            [
                jnp.where(
                    first,
                    mix[b0 * square + c * components + d],
                    mix[b1 * square + c * components + d],
                )
                for d in range(components)
            ]
            for c in range(components)
        ]
        out_ref[m] = mix_rows(weights, coef, components).astype(jnp.bfloat16)

    for out_ref, offset in zip(outs, offsets):
        g = jnp.bitwise_xor(me[0], offset)
        used = count[g]

        def several(step, carry, out_ref=out_ref, g=g, used=used):
            for u in range(unroll):
                one(out_ref, g, used, step * unroll + u)
            return carry

        steps = (used + 2 * unroll - 1) // (2 * unroll)
        lax.fori_loop(0, steps, several, 0)

        def blank(m, carry, out_ref=out_ref):
            out_ref[m] = jnp.zeros((channels, lanes), jnp.bfloat16)
            return carry

        lax.fori_loop(steps * unroll, pairs, blank, 0)


def near_kernel(components, near_src, near_tgt, near_mix, field_ref, matrix_ref, out_ref, x_ref):
    channels = out_ref.shape[1]
    square = components * components
    split_clusters(field_ref, x_ref)
    out_ref[...] = jnp.zeros_like(out_ref)
    for n in range(matrix_ref.shape[0]):
        x = x_ref[pl.ds(pl.multiple_of(near_src[n] * channels, 32), channels), :]
        y = lax.dot_general(x, matrix_ref[n], NT, preferred_element_type=jnp.float32)
        weights = [
            [near_mix[n * square + c * components + d] for d in range(components)]
            for c in range(components)
        ]
        out_ref[near_tgt[n]] += mix_rows(weights, y, components)


def far_kernel(offset, pair_total, me, cluster, near_ref, got_ref, u_ref, out_ref, *rounded):
    step = pl.program_id(0)
    pairs, channels, lanes = got_ref.shape
    first = lax.broadcasted_iota(jnp.int32, (channels, lanes), 1) < lanes // 2
    unroll = 4 if pairs % 4 == 0 else 1
    base = jnp.bitwise_xor(me[0], offset) * pair_total + step * pairs

    @pl.when(step == 0)
    def _():
        out_ref[...] = near_ref[...]

    def several(at, carry):
        done = []
        for u in range(unroll):
            m = at * unroll + u
            a = got_ref[m]
            zero = jnp.zeros_like(a)
            both = jnp.concatenate(
                [jnp.where(first, a, zero), jnp.where(first, zero, a)], axis=0
            )
            done.append(
                jnp.dot(both, u_ref[m], preferred_element_type=jnp.float32)
            )
        for u in range(unroll):
            k = 2 * (base + at * unroll + u)
            out_ref[cluster[k]] += done[u][:channels]
            out_ref[cluster[k + 1]] += done[u][channels:]
        return carry

    lax.fori_loop(0, pairs // unroll, several, 0)

    if rounded:

        @pl.when(step == pl.num_programs(0) - 1)
        def _():
            rounded[0][...] = out_ref[...].astype(jnp.bfloat16)


def body(
    field,
    dest_group,
    src_local,
    ranks,
    mixing,
    v_factor,
    u_factor,
    slot_cluster,
    near_src,
    near_tgt,
    near_mixing,
    near_matrix,
):
    groups = lax.axis_size("tgt")
    shards = lax.axis_size("src")
    pairing = lax.axis_size("comp")
    blocks, rank_width, cluster_size = v_factor.shape
    components, vectors, points = field.shape
    channels = components * vectors
    owned = points // cluster_size
    slot_count = u_factor.shape[0]
    capacity = slot_count // groups
    pairs = capacity // 2
    targets = owned * shards
    sources = field.reshape(channels, points)
    smem = pl.BlockSpec(memory_space=pltpu.SMEM)
    vmem = pl.BlockSpec(memory_space=pltpu.VMEM)
    lanes = 2 * rank_width
    me = lax.axis_index("tgt").astype(jnp.int32).reshape(1)
    destination = dest_group.reshape(-1)
    flat_mixing = mixing.reshape(-1)

    def coefficients(offsets):
        size = len(offsets) * blocks // groups
        return pl.pallas_call(
            functools.partial(coef_kernel, components, groups, offsets),
            out_shape=[
                jax.ShapeDtypeStruct((pairs, channels, lanes), jnp.bfloat16) for _ in offsets
            ],
            in_specs=[smem] * 5 + [vmem] * 2,
            out_specs=[vmem] * len(offsets),
            scratch_shapes=[
                pltpu.VMEM((owned * channels, cluster_size), jnp.bfloat16),
                pltpu.SMEM((slot_count,), jnp.int32),
                pltpu.SMEM((groups,), jnp.int32),
            ],
            cost_estimate=pl.CostEstimate(
                flops=16 * size * rank_width * cluster_size * channels,
                bytes_accessed=2 * v_factor.size,
                transcendentals=0,
            ),
            name="coef",
        )(me, destination, src_local, ranks, flat_mixing, sources, v_factor)

    def pass_on(value, offset):
        return lax.ppermute(value, "tgt", [(i, i ^ offset) for i in range(groups)])

    early = list(range(1, groups // 2 + 1))
    late = list(range(groups // 2 + 1, groups)) + [0]
    passed = {}
    for offset, value in zip(early, coefficients(early)):
        passed[offset] = pass_on(value, offset)
    for offset, value in zip(late, coefficients(late)):
        passed[offset] = pass_on(value, offset) if offset else value

    total = pl.pallas_call(
        functools.partial(near_kernel, components),
        out_shape=jax.ShapeDtypeStruct((targets, channels, cluster_size), jnp.float32),
        in_specs=[smem] * 3 + [vmem] * 2,
        out_specs=vmem,
        scratch_shapes=[pltpu.VMEM((owned * channels, cluster_size), jnp.bfloat16)],
        cost_estimate=pl.CostEstimate(
            flops=2 * near_matrix.size * channels, bytes_accessed=3000000, transcendentals=0
        ),
        name="near",
    )(near_src, near_tgt, near_mixing.reshape(-1), sources, near_matrix)

    chunk = 16 if pairs % 16 == 0 else pairs
    steps = pairs // chunk
    bases = u_factor.reshape(slot_count // 2, lanes, cluster_size)
    whole = (targets, channels, cluster_size)
    for offset in [0] + early + late[:-1]:
        final = offset == groups - 1

        def tile(i, me_ref, cluster_ref, offset=offset):
            return (jnp.bitwise_xor(me_ref[0], offset) * steps + i, 0, 0)

        results = pl.pallas_call(
            functools.partial(far_kernel, offset, pairs),
            grid_spec=pltpu.PrefetchScalarGridSpec(
                num_scalar_prefetch=2,
                grid=(steps,),
                in_specs=[
                    vmem,
                    pl.BlockSpec((chunk, channels, lanes), lambda i, *_: (i, 0, 0)),
                    pl.BlockSpec((chunk, lanes, cluster_size), tile),
                ],
                out_specs=[vmem] * (1 + final),
            ),
            out_shape=[
                jax.ShapeDtypeStruct(whole, kind)
                for kind in (jnp.float32, jnp.bfloat16)[: 1 + final]
            ],
            compiler_params=pltpu.CompilerParams(dimension_semantics=("arbitrary",)),
            cost_estimate=pl.CostEstimate(
                flops=16 * pairs * lanes * cluster_size * channels,
                bytes_accessed=2 * pairs * lanes * cluster_size,
                transcendentals=0,
            ),
            name="far",
        )(me, slot_cluster, total, passed[offset], bases)
        total = results[0]

    members = pairing * shards
    kept = targets // members
    pieces = total.reshape(members, kept, channels, cluster_size)
    arrived = lax.all_to_all(
        results[1].reshape(pieces.shape), ("comp", "src"), split_axis=0, concat_axis=0, tiled=True
    )
    at = lax.axis_index("comp") * shards + lax.axis_index("src")
    own = lax.dynamic_index_in_dim(pieces, at, 0, keepdims=False)
    other = (jnp.arange(members) != at)[:, None, None, None]
    summed = own + jnp.sum(jnp.where(other, arrived.astype(jnp.float32), 0.0), axis=0)
    return summed.transpose(1, 0, 2).reshape(components, vectors, kept * cluster_size)


def solution(mesh):
    placed = (
        P(None, None, ("tgt", "src")),
        P(("comp", "tgt", "src"), None),
        P(("comp", "tgt", "src")),
        P(("comp", "tgt", "src")),
        P(("comp", "tgt", "src"), None, None),
        P(("comp", "tgt", "src"), None, None),
        P(("comp", "tgt", "src"), None, None),
        P(("comp", "tgt", "src")),
        P(("comp", "tgt", "src")),
        P(("comp", "tgt", "src")),
        P(("comp", "tgt", "src"), None, None),
        P(("comp", "tgt", "src"), None, None),
    )
    return jax.shard_map(
        body,
        mesh=mesh,
        in_specs=placed,
        out_specs=P(None, None, ("comp", "tgt", "src")),
        check_vma=False,
    )
```
